128 devices in a mesh: dp: 16 (over y, z), vocab: 8 (over x, core).
Axes of the slice: x: 4, y: 4, z: 4, core: 2. Of those that a mesh axis runs over, the one named last changes fastest.
Arguments:
- tokens: bfloat16 [2048, 7168], P('dp'), may hold values from -6 to 6
- expert_hidden: bfloat16 [2048, 8, 1024], P('dp'), may hold values from -6 to 6
- routes: int32 [2048, 8], P('dp'), may hold values from 0 to 63, all different within a row; in each aligned block of 16 rows (0 to 15, 16 to 31, ...) at most 3 rows name the same one
- route_weight: float32 [2048, 8], P('dp'), may hold values from 0.05 to 0.45
- expert_weight: bfloat16 [128, 512, 7168], P(('dp', 'vocab')), may hold values from -0.1875 to 0.1875
- norm_gain: float32 [7168], replicated, may hold values from 0.5 to 1.5
- head_weight: bfloat16 [7168, 114688], P(None, ('dp', 'vocab')), may hold values from -8 to 8
- targets: int32 [2048], P('dp'), may hold values from 0 to 114687
- rollout_logprob: float32 [2048], P('dp'), may hold values from -21 to -13
- advantages: float32 [2048], P('dp'), may hold values from -5 to 5
Outputs:
- layer_out: bfloat16 [2048, 7168], P('dp')
- token_logprob: float32 [2048], P('dp')
- token_loss: float32 [2048], P('dp')
The draws below stay inside these ranges and needn't reach their ends.
Inputs may be any that keep to these rules, and one draw needn't show every extreme that they name: The 8 routes of a token name different experts; among the routes of one aligned block of 16 token rows, no expert is named more than 3 times.
All inputs are finite; a program needn't handle non-finite values.
Results may differ from the reference program's by a relative error of at most 0.02.
Values may be sent and summed in bfloat16 or wider, within the bound.
No kernel may reach another device: no remote copies, remote signals or barrier semaphores. Data moves between devices by JAX's collectives and lax.ppermute only.
A program may use at most 192 MiB of HBM per device.

```python
import math
import jax
import jax.numpy as jnp
import numpy as np
from jax import lax

D = 7168
HE = 1024
TOPK = 8
VOCAB = 114688
EXPERTS = 64
SUB = 16
CAP = 3
TOKENS = 2048


def draw_head_weight(key, part):
    first, second = jax.random.split(key, 2)
    columns = jnp.arange(VOCAB, dtype=jnp.float32)
    rough = jnp.exp(jax.random.uniform(first, (VOCAB,), jnp.float32, jnp.log(0.7), jnp.log(1.4)))
    scale = (1.5 + 2.5 * columns / VOCAB) * rough / jnp.sqrt(jnp.float32(D))
    values = jax.random.normal(second, (D, VOCAB), jnp.float32) * scale[None, :]
    values = jnp.clip(values, -8.0, 8.0)
    return values.astype(jnp.bfloat16)


def with_ends(drawn, stream_key, low, largest):
    longest = drawn.shape.index(max(drawn.shape))
    spots = []
    for shift in (0, 1):
        where = [jax.random.randint(jax.random.fold_in(stream_key, axis), (), 0, length) for axis, length in enumerate(drawn.shape)]
        where[longest] = (where[longest] + shift) % drawn.shape[longest]
        spots.append(tuple(where))
    return drawn.at[spots[0]].set(low).at[spots[1]].set(largest)


def shard_levels(own_key, dims, shards, low, top_value):
    def one(position, blocks):
        draws = jax.random.uniform(jax.random.fold_in(jax.random.fold_in(own_key, 6), position), (blocks,), jnp.float32, low / len(shards), top_value / len(shards))
        return jnp.repeat(jnp.exp(draws), dims[position] // blocks).reshape((-1,) + (1,) * (len(dims) - position - 1))

    loudness = one(*shards[0])
    for cut in shards[1:]:
        loudness = loudness * one(*cut)
    return loudness


def assign_block(rng, own, number, rows, amount, top, reach, lean):
    sequence = jax.random.permutation(rng, amount)
    packed, usual = load_shares(amount, rows * top, reach, lean, True), load_shares(amount, rows * top, reach, lean, False)
    places = jnp.arange(amount)

    def named(tallies, rotation):
        used = int((tallies > 0).sum())
        fixed = max(1, used // 4)
        passed = fixed + (places - fixed + rotation * (used - fixed)) % max(1, amount - fixed)
        return jnp.zeros((amount,), jnp.int32).at[sequence[jnp.where(places < fixed, places, passed)]].set(jnp.asarray(tallies, jnp.int32))

    tallies = jnp.where(number % 4 == 0, named(packed, number // 4), named(usual, number - number // 4 - 1))
    mixed = jax.random.permutation(jax.random.fold_in(own, 3), amount)
    source_of, sink = mixed[0:amount // 2 * 2:2], mixed[1:amount // 2 * 2:2]
    room = jnp.minimum(tallies[source_of] - 1, reach - tallies[sink]) // 2
    room = jnp.where((source_of == sequence[0]) | (sink == sequence[0]) | (tallies[sink] == 0), 0, jnp.maximum(room, 0))
    passed = jax.random.randint(jax.random.fold_in(own, 4), (amount // 2,), 0, 1 << 20) % (room + 1)
    tallies = tallies.at[source_of].add(-passed).at[sink].add(passed)
    items = jnp.searchsorted(jnp.cumsum(tallies), jnp.arange(rows * top), side="right").astype(jnp.int32)
    listing = items.reshape(top, rows).T
    listing = listing[jax.random.permutation(jax.random.fold_in(own, 1), rows)]
    rotation = jax.random.randint(jax.random.fold_in(own, 2), (rows, 1), 0, top)
    return jnp.take_along_axis(listing, (jnp.arange(top)[None, :] + rotation) % top, axis=1)


def load_shares(number_of, total, most, skew, full):
    portions = [(1 << 20) // math.isqrt(rank ** skew) + 1 for rank in range(1, number_of + 1)]
    largest = most if full else min(most, max(-(-total // number_of), total * portions[0] // sum(portions)))
    least = 1 if total - largest >= number_of - 1 else 0
    holding, spare = [largest] + [least] * (number_of - 1), total - largest - least * (number_of - 1)
    while spare > 0:
        movable = [i for i in range(1, number_of) if holding[i] < largest] or [i for i in range(1, number_of) if holding[i] < most]
        whole, budget = sum([portions[i] for i in movable]), spare
        for i in movable:
            more = min(most - holding[i], max(1, budget * portions[i] // whole), spare)
            holding[i] = holding[i] + more
            spare = spare - more
    return np.array(holding)


def bell_draw(key, shape, scale, limit, cuts=(), kind=jnp.bfloat16):
    result = jax.random.normal(key, shape, jnp.float32) * scale
    if len(cuts) > 0:
        result = shard_levels(key, shape, cuts, -0.22, 0.18) * result
    return jnp.clip(result, min=-limit, max=limit).astype(kind)


def setup_inputs(seed: int = 0) -> dict:
    keys = jax.random.split(jax.random.key(seed), 11)
    tokens = bell_draw(keys[0], (TOKENS, D), 1.0, 6.0, ((0, 16),))
    expert_hidden = bell_draw(keys[1], (TOKENS, TOPK, HE), 1.0, 6.0, ((0, 16),))
    routes_keys = jax.random.split(jax.random.fold_in(keys[2], 1), TOKENS // SUB)
    routes_turns = jax.random.permutation(jax.random.fold_in(keys[2], 3), TOKENS // SUB)
    routes = jax.vmap(lambda own, number: assign_block(jax.random.fold_in(keys[2], 2), own, number, SUB, EXPERTS, TOPK, CAP, 2))(routes_keys, routes_turns).reshape((TOKENS, TOPK))
    route_weight = jnp.clip(0.05 + 0.39999999 * jax.random.uniform(keys[3], (TOKENS, TOPK), jnp.float32) ** shard_levels(keys[3], (TOKENS, TOPK), ((0, 16),), -0.2, 0.2), 0.05, 0.45)
    expert_weight = bell_draw(keys[4], (2 * EXPERTS, HE // 2, D), HE ** -0.5, 0.1875, ((0, 128),))
    norm_gain = jnp.clip(1.0 + 0.1 * jax.random.normal(keys[5], (D,), jnp.float32), 0.5, 1.5)
    head_weight = draw_head_weight(jax.random.fold_in(keys[10], 71), 0)
    targets = with_ends(jax.random.randint(keys[7], (TOKENS,), 0, VOCAB), jax.random.fold_in(keys[7], 1), 0, VOCAB - 1).astype(jnp.int32)
    rollout_logprob = jnp.clip(-21.0 + 8.0 * jax.random.uniform(keys[8], (TOKENS,), jnp.float32) ** shard_levels(keys[8], (TOKENS,), ((0, 16),), -0.2, 0.2), -21.0, -13.0)
    advantages = bell_draw(keys[9], (TOKENS,), 1.0, 5.0, ((0, 16),), jnp.float32)
    return {"tokens": tokens, "expert_hidden": expert_hidden, "routes": routes, "route_weight": route_weight, "expert_weight": expert_weight, "norm_gain": norm_gain, "head_weight": head_weight, "targets": targets, "rollout_logprob": rollout_logprob, "advantages": advantages}


norm_epsilon = 1e-06
clip_low = 0.8
clip_high = 1.2
dual_bound = 3.0

def rms_scale(values, norm_gain):
    widened = values.astype(jnp.float32)
    mean_square = lax.optimization_barrier(jnp.mean(widened * widened, axis=-1, keepdims=True))
    return (widened * lax.rsqrt(mean_square + norm_epsilon) * norm_gain).astype(jnp.bfloat16)

def clipped_loss(logprob, rollout_logprob, advantages):
    ratio = jnp.exp(logprob - rollout_logprob)
    surrogate = jnp.minimum(ratio * advantages, jnp.clip(ratio, clip_low, clip_high) * advantages)
    bounded = jnp.where(advantages < 0.0, jnp.maximum(surrogate, dual_bound * advantages), surrogate)
    return -bounded

def apply_expert(operands):
    rows_in, weight = operands
    half_width = rows_in.shape[1] // 2
    lower_part = jnp.dot(rows_in[:, :half_width], weight[:half_width], preferred_element_type=jnp.float32).astype(jnp.bfloat16)
    upper_part = jnp.dot(rows_in[:, half_width:], weight[half_width:], preferred_element_type=jnp.float32).astype(jnp.bfloat16)
    return (lower_part, upper_part)

def reference(tokens, expert_hidden, routes, route_weight, expert_weight, norm_gain, head_weight, targets, rollout_logprob, advantages):
    blocks = TOKENS // SUB
    routes_blocked = routes.reshape(blocks, SUB * TOPK)
    onehot = (routes_blocked[:, :, None] == jnp.arange(EXPERTS, dtype=jnp.int32)[None, None, :]).astype(jnp.int32)
    before = jnp.cumsum(onehot, axis=1) - onehot
    slot_index = lax.optimization_barrier(jnp.sum(before * onehot, axis=2))
    buffer_row = (jnp.arange(blocks, dtype=jnp.int32)[:, None] * CAP + slot_index).reshape(-1).astype(jnp.int32)
    expert_ids = routes_blocked.reshape(-1).astype(jnp.int32)
    hidden_rows = expert_hidden.reshape(-1, HE)
    buffer = jnp.zeros((EXPERTS, blocks * CAP, HE), expert_hidden.dtype).at[expert_ids, buffer_row].set(hidden_rows)
    weights_full = expert_weight.reshape(EXPERTS, HE, D)
    lower_out, upper_out = lax.map(apply_expert, (buffer, weights_full))
    route_out = lower_out[expert_ids, buffer_row].astype(jnp.float32) + upper_out[expert_ids, buffer_row].astype(jnp.float32)
    route_out = route_out.reshape(TOKENS, TOPK, D)
    moe = lax.optimization_barrier(jnp.sum(route_out * route_weight[:, :, None], axis=1))
    layer_out = (tokens.astype(jnp.float32) + moe).astype(jnp.bfloat16)
    normed = rms_scale(layer_out, norm_gain)
    logits = jnp.dot(normed, head_weight, preferred_element_type=jnp.float32)
    row_peak = lax.optimization_barrier(jnp.max(logits, axis=1))
    log_total = row_peak + jnp.log(lax.optimization_barrier(jnp.sum(jnp.exp(logits - row_peak[:, None]), axis=1)))
    target_logit = jnp.take_along_axis(logits, targets[:, None].astype(jnp.int32), axis=1)[:, 0]
    token_logprob = target_logit - log_total
    token_loss = clipped_loss(token_logprob, rollout_logprob, advantages)
    return (layer_out, token_logprob, token_loss)
```

```python
import jax
import jax.numpy as jnp
from jax import lax
from jax.sharding import Mesh
from jax.sharding import PartitionSpec as P

X = "vocab_0"
CORE = "vocab_1"
VOCAB = ("vocab_0", "vocab_1")
DP_VOCAB = ("dp_0", "dp_1", "vocab_0", "vocab_1")
DP = ("dp_0", "dp_1")

norm_epsilon = 1e-06
clip_low = 0.8
clip_high = 1.2
dual_bound = 3.0
bf16 = jnp.bfloat16
f32 = jnp.float32


def clipped_loss(logprob, rollout_logprob, advantages):
    ratio = jnp.exp(logprob - rollout_logprob)
    surrogate = jnp.minimum(ratio * advantages, jnp.clip(ratio, clip_low, clip_high) * advantages)
    bounded = jnp.where(
        advantages < 0.0, jnp.maximum(surrogate, dual_bound * advantages), surrogate
    )
    return -bounded


def dot(a, b):
    return jnp.dot(a, b, preferred_element_type=f32)


def swap_cores(x):
    return lax.ppermute(x, CORE, [(0, 1), (1, 0)])


def label_row(targets):
    digits = [(targets // 128**k) % 128 for k in range(3)]
    row = jnp.concatenate(digits + [jnp.zeros_like(targets)]).astype(bf16)
    return row[None]


def labels_of(rows):
    digits = rows.astype(f32).astype(jnp.int32).reshape(rows.shape[0], 4, 128)
    return digits[:, 0] + 128 * digits[:, 1] + 128 * 128 * digits[:, 2]


def experts_stage(tokens, expert_hidden, routes, route_weight, expert_weight, targets):
    x, h = lax.axis_index(X), lax.axis_index(CORE)
    rows, top = routes.shape
    width = expert_hidden.shape[2] // 2
    cols = tokens.shape[1] // 2
    blocks = rows // 16
    by_block = routes.reshape(blocks, 16 * top).T
    mine = (
        by_block[:, :, None] == (lax.iota(jnp.int32, 16) * 4 + x)[None, None, :]
    ).astype(bf16)
    n = 16 * top
    lower = (lax.iota(jnp.int32, n)[:, None] > lax.iota(jnp.int32, n)[None, :]).astype(bf16)
    before = dot(lower, mine.reshape(n, blocks * 16)).reshape(n, blocks, 16)
    slot = jnp.sum(before * mine.astype(f32), axis=2).astype(jnp.int32)
    place = (by_block // 4) * 24 + lax.iota(jnp.int32, blocks)[None, :] * 3 + slot
    place = jnp.where(by_block % 4 == x, place, -1).T.reshape(rows, top)
    select = (lax.iota(jnp.int32, 384)[:, None] == place.reshape(-1)[None, :]).astype(bf16)
    hidden = lax.dynamic_slice_in_dim(
        expert_hidden.reshape(rows * top, 2 * width), h * width, width, 1
    )
    buffer = dot(select, hidden).astype(bf16).reshape(16, 24, width)
    extra = jnp.pad(label_row(targets), ((0, 7), (0, 0)))
    buffer = jnp.concatenate(
        [buffer, jnp.broadcast_to(extra[None], (16, 8, width))], axis=1
    )
    received = lax.all_to_all(buffer, DP, 0, 0, tiled=True)
    labels = labels_of(received[:, 24])
    own = received[:, :24].reshape(384, width)
    other = swap_cores(own)
    weight = expert_weight[0]
    weight_own = lax.dynamic_slice_in_dim(weight, h * cols, cols, 1)
    weight_other = swap_cores(lax.dynamic_slice_in_dim(weight, (1 - h) * cols, cols, 1))
    product = (dot(own, weight_own) + dot(other, weight_other)).astype(bf16)
    back = lax.all_to_all(product.reshape(16, 24, cols), DP, 0, 0, tiled=True)
    gate = jnp.sum(
        jnp.where(
            place[:, :, None] == lax.iota(jnp.int32, 384)[None, None, :],
            route_weight[:, :, None],
            0.0,
        ),
        axis=1,
    )
    gate_high = gate.astype(bf16)
    gate_low = (gate - gate_high.astype(f32)).astype(bf16)
    both = dot(jnp.concatenate([gate_high, gate_low]), back.reshape(384, cols))
    partial = (both[:rows] + both[rows:]).astype(bf16)
    parts = lax.all_to_all(partial.reshape(4, rows // 4, cols), X, 0, 0, tiled=True)
    moe = jnp.sum(parts.astype(f32), axis=0)
    mine_tokens = lax.dynamic_slice(tokens, (x * (rows // 4), h * cols), (rows // 4, cols))
    return (mine_tokens.astype(f32) + moe).astype(bf16), labels


def combined(peaks, totals, picks):
    peak = jnp.max(peaks, axis=0)
    return peak, jnp.sum(totals * jnp.exp(peaks - peak), axis=0), jnp.sum(picks, axis=0)


def per_device(
    tokens,
    expert_hidden,
    routes,
    route_weight,
    expert_weight,
    norm_gain,
    head_weight,
    targets,
    rollout_logprob,
    advantages,
):
    h = lax.axis_index(CORE)
    tile, labels = experts_stage(
        tokens, expert_hidden, routes, route_weight, expert_weight, targets
    )
    sub, cols = tile.shape[0] // 2, tile.shape[1]
    kept = lax.dynamic_slice_in_dim(tile, h * sub, sub, 0)
    got = swap_cores(lax.dynamic_slice_in_dim(tile, (1 - h) * sub, sub, 0))
    layer_sub = jnp.where(
        h == 0, jnp.concatenate([kept, got], axis=1), jnp.concatenate([got, kept], axis=1)
    )
    group_layer = lax.all_to_all(
        jnp.broadcast_to(layer_sub[None], (8, *layer_sub.shape)), VOCAB, 0, 0, tiled=True
    ).reshape(tokens.shape)
    widened = layer_sub.astype(f32)
    mean_square = jnp.mean(widened * widened, axis=-1, keepdims=True)
    normed_sub = (widened * lax.rsqrt(mean_square + norm_epsilon) * norm_gain).astype(bf16)
    voc_dev = head_weight.shape[1]
    columns = lax.axis_index(DP_VOCAB) * voc_dev + lax.iota(jnp.int32, voc_dev)
    by_device = labels.reshape(-1, 2, sub // 2)
    stats = []
    for c in range(2):
        piece = normed_sub[c * (sub // 2) : (c + 1) * (sub // 2)]
        normed = lax.all_gather(piece, DP_VOCAB, axis=0, tiled=True)
        logits = dot(normed, head_weight)
        peak = jnp.max(logits, axis=1)
        total = jnp.sum(jnp.exp(logits - peak[:, None]), axis=1)
        wanted = by_device[:, c].reshape(-1)
        picked = jnp.sum(jnp.where(columns[None, :] == wanted[:, None], logits, 0.0), axis=1)
        stats.append(jnp.stack([peak, total, picked]).reshape(3, -1, 1, sub // 2))
    stats = jnp.concatenate(stats, axis=2).reshape(3, 16, -1).transpose(1, 0, 2)
    sent = lax.all_to_all(stats, DP, 0, 0, tiled=True)
    group = jnp.stack(combined(sent[:, 0], sent[:, 1], sent[:, 2]))
    sent = lax.all_gather(group, VOCAB, axis=0)
    peak, total, target_logit = combined(sent[:, 0], sent[:, 1], sent[:, 2])
    token_logprob = target_logit - (peak + jnp.log(total))
    token_loss = clipped_loss(token_logprob, rollout_logprob, advantages)
    return (group_layer, token_logprob, token_loss)


def solution(mesh):
    torus = Mesh(mesh.devices.reshape(4, 4, 4, 2), ("dp_0", "dp_1", "vocab_0", "vocab_1"))
    placed = (
        P(DP, None),
        P(DP, None, None),
        P(DP, None),
        P(DP, None),
        P(DP_VOCAB, None, None),
        P(),
        P(None, DP_VOCAB),
        P(DP),
        P(DP),
        P(DP),
    )
    return jax.shard_map(
        per_device,
        mesh=torus,
        in_specs=placed,
        out_specs=(P(DP, None), P(DP), P(DP)),
        check_vma=False,
    )
```

```python
import functools

import jax
import jax.numpy as jnp
from jax import lax
from jax.experimental import pallas as pl
from jax.experimental.pallas import tpu as pltpu
from jax.sharding import Mesh
from jax.sharding import PartitionSpec as P

X = "vocab_0"
Y = "dp_0"
Z = "dp_1"
CORE = "vocab_1"
VOCAB = ("vocab_0", "vocab_1")
DP_VOCAB = ("dp_0", "dp_1", "vocab_0", "vocab_1")
DP = ("dp_0", "dp_1")

norm_epsilon = 1e-06
clip_low = 0.8
clip_high = 1.2
dual_bound = 3.0
bf16 = jnp.bfloat16
f32 = jnp.float32

PARTS = ((0, 1152), (1152, 1152), (2304, 1280))
ORDERS = ((X, Y, Z), (Y, Z, X), (Z, X, Y))
EXTRA = 128
TILE = 32


def clipped_loss(logprob, rollout_logprob, advantages):
    ratio = jnp.exp(logprob - rollout_logprob)
    surrogate = jnp.minimum(ratio * advantages, jnp.clip(ratio, clip_low, clip_high) * advantages)
    bounded = jnp.where(
        advantages < 0.0, jnp.maximum(surrogate, dual_bound * advantages), surrogate
    )
    return -bounded


def dot(a, b):
    return jnp.dot(a, b, preferred_element_type=f32)


def moved(x, axis, step):
    n = lax.axis_size(axis)
    return lax.ppermute(x, axis, [(i, (i + step) % n) for i in range(n)])


def swap_cores(x):
    return lax.ppermute(x, CORE, [(0, 1), (1, 0)])


def bf16_terms(x):
    terms = []
    for _ in range(3):
        term = lax.reduce_precision(x, 8, 7)
        terms.append(term)
        x = x - term
    return terms


def experts_stage(tokens, expert_hidden, routes, route_weight, expert_weight, beside):
    x, h = lax.axis_index(X), lax.axis_index(CORE)
    rows, top = routes.shape
    width = expert_hidden.shape[2] // 2
    cols = tokens.shape[1] // 2
    blocks = rows // 16
    by_block = routes.reshape(blocks, 16 * top).T
    mine = (
        by_block[:, :, None] == (lax.iota(jnp.int32, 16) * 4 + x)[None, None, :]
    ).astype(bf16)
    n = 16 * top
    lower = (lax.iota(jnp.int32, n)[:, None] > lax.iota(jnp.int32, n)[None, :]).astype(bf16)
    before = dot(lower, mine.reshape(n, blocks * 16)).reshape(n, blocks, 16)
    slot = jnp.sum(before * mine.astype(f32), axis=2).astype(jnp.int32)
    place = (by_block // 4) * 24 + lax.iota(jnp.int32, blocks)[None, :] * 3 + slot
    place = jnp.where(by_block % 4 == x, place, -1).T.reshape(rows, top)
    select = (lax.iota(jnp.int32, 384)[:, None] == place.reshape(-1)[None, :]).astype(bf16)
    picked = dot(select, expert_hidden.reshape(rows * top, 2 * width)).astype(bf16)
    buffer = lax.dynamic_slice_in_dim(picked, h * width, width, 1).reshape(16, 24, width)
    own = lax.all_to_all(buffer, DP, 0, 0, tiled=True).reshape(384, width)
    other = swap_cores(own)
    weight = expert_weight[0]
    weight_own = lax.dynamic_slice_in_dim(weight, h * cols, cols, 1)
    weight_other = lax.dynamic_slice_in_dim(swap_cores(weight), h * cols, cols, 1)
    product = (dot(own, weight_own) + dot(other, weight_other)).astype(bf16)
    back = lax.all_to_all(product.reshape(16, 24, cols), DP, 0, 0, tiled=True)
    back, beside = lax.optimization_barrier((back, beside(product)))
    gate = jnp.sum(
        jnp.where(
            place[:, :, None] == lax.iota(jnp.int32, 384)[None, None, :],
            route_weight[:, :, None],
            0.0,
        ),
        axis=1,
    )
    high, low, _ = bf16_terms(gate)
    both = dot(jnp.concatenate([high, low]).astype(bf16), back.reshape(384, cols))
    partial = (both[:rows] + both[rows:]).astype(bf16)
    parts = lax.all_to_all(partial.reshape(4, rows // 4, cols), X, 0, 0, tiled=True)
    moe = jnp.sum(parts.astype(f32), axis=0)
    mine_tokens = lax.dynamic_slice(tokens, (x * TILE, h * cols), (TILE, cols))
    return (mine_tokens.astype(f32) + moe).astype(bf16), beside


def extra_columns(tile, labels):
    wide = tile.astype(f32)
    squares = jnp.sum(wide * wide, axis=1)
    lanes = bf16_terms(squares + swap_cores(squares))
    lanes += [((labels // 128**k) % 128).astype(f32) for k in range(3)]
    lane = lax.broadcasted_iota(jnp.int32, (TILE, EXTRA), 1)
    out = jnp.zeros((TILE, EXTRA), f32)
    for k, value in enumerate(lanes):
        out = jnp.where(lane == k, value[:, None], out)
    return out.astype(bf16)


def rows_of(part, j3, j2, j1):
    if part == 0:
        return j2, j3, j1
    if part == 1:
        return j1, j2, j3
    return j3, j1, j2


def head_kernel(items, first, *refs):
    count = len(items)
    lhs, (head_theirs, head_mine), rest = refs[:count], refs[count : count + 2], refs[count + 2 :]
    if not first:
        sums_in, rest = rest[:2], rest[2:]
    sums, bufs, sems = rest[:2], rest[2 : 2 + count], rest[2 + count]
    step = pl.program_id(0)
    copies = [
        pltpu.make_async_copy(src, buf, sems.at[k]) for k, (src, buf) in enumerate(zip(lhs, bufs))
    ]

    @pl.when(step == 0)
    def _():
        for copy in copies:
            copy.start()

    for k in range(2):
        sums[k][...] = jnp.zeros_like(sums[k]) if first else sums_in[k][...]

    @pl.when(step == 0)
    def _():
        for copy in copies:
            copy.wait()

    for k, (part, j3, j2_first) in enumerate(items):
        start, width = PARTS[part]
        rhs = jnp.concatenate(
            [head_theirs[0, start : start + width], head_mine[0, start : start + width]], axis=1
        )
        result = dot(bufs[k][:, :width], rhs)
        for b in range(8):
            jy, jz, jx = rows_of(part, j3, j2_first + b // 4, b % 4)
            rows = slice(b * TILE, (b + 1) * TILE)
            for side in range(2):
                sums[side][0, jy, jz, jx] += result[rows, side * 128 : side * 128 + 128]


def head_call(items, lhs, heads, sums):
    tiles, depth, _ = heads[0].shape
    any_spec = pl.BlockSpec(memory_space=pl.ANY)
    head_spec = pl.BlockSpec((1, depth, 128), lambda n: (n, 0, 0))
    sum_spec = pl.BlockSpec((1, 4, 4, 4, TILE, 128), lambda n: (n, 0, 0, 0, 0, 0))
    sum_shape = jax.ShapeDtypeStruct((tiles, 4, 4, 4, TILE, 128), f32)
    first = sums is None
    sums = () if first else sums
    size = sum(a.size for a in lhs)
    return pl.pallas_call(
        functools.partial(head_kernel, items, first),
        grid=(tiles,),
        in_specs=[any_spec] * len(lhs) + [head_spec] * 2 + [sum_spec] * len(sums),
        out_specs=[sum_spec] * 2,
        out_shape=[sum_shape] * 2,
        scratch_shapes=[
            *[pltpu.VMEM(a.shape, a.dtype) for a in lhs],
            pltpu.SemaphoreType.DMA((len(lhs),)),
        ],
        cost_estimate=pl.CostEstimate(
            flops=2 * size * tiles * 256,
            bytes_accessed=2 * size + 2 * heads[0].size * 2 + (2 + len(sums)) * 4 * tiles * 2048 * 128,
            transcendentals=0,
        ),
        compiler_params=pltpu.CompilerParams(
            dimension_semantics=("arbitrary",), vmem_limit_bytes=56 * 1024 * 1024
        ),
    )(*lhs, *heads, *sums)


def stats_kernel(dim, spots, places, mine, theirs, *refs):
    count = len(spots)
    sources, out, extra, sems = refs[:count], refs[count], refs[count + 1], refs[count + 2]
    block = pl.program_id(0)
    jy, jz = block // 4, block % 4
    copies = [
        pltpu.make_async_copy(
            src.at[:, pl.ds(PARTS[0][1], EXTRA)], extra.at[j3, pl.ds(row, 256)], sems.at[k]
        )
        for k, (src, (j3, row)) in enumerate(zip(sources, spots))
    ]

    @pl.when(block == 0)
    def _():
        for copy in copies:
            copy.start()
        for copy in copies:
            copy.wait()

    fields = extra[jz, pl.ds(pl.multiple_of(jy * 128, 128), 128), :].astype(f32)
    squares = fields[:, 0:1] + fields[:, 1:2] + fields[:, 2:3]
    scale = lax.rsqrt(squares / dim + norm_epsilon)
    label = fields[:, 3:4] + 128.0 * fields[:, 4:5] + 16384.0 * fields[:, 5:6]
    wanted = label.astype(jnp.int32) - places[3]
    tiles = [
        (mine[t].reshape(128, 128) + theirs[t].reshape(128, 128)) * scale
        for t in range(mine.shape[0])
    ]
    peak = jnp.max(functools.reduce(jnp.maximum, tiles), axis=1, keepdims=True)
    total = functools.reduce(jnp.add, [jnp.exp(v - peak) for v in tiles])
    lane = lax.broadcasted_iota(jnp.int32, (128, 128), 1)
    pick = functools.reduce(
        jnp.add, [jnp.where(lane + 128 * t == wanted, v, 0.0) for t, v in enumerate(tiles)]
    )
    total = jnp.sum(total, axis=1, keepdims=True)
    pick = jnp.sum(pick, axis=1, keepdims=True)
    three = jnp.where(lane == 0, peak, jnp.where(lane == 1, total, pick))
    group = lax.rem(places[0] + jy, 4) * 4 + lax.rem(places[1] + jz, 4)
    out[group] = pltpu.roll(three.T[:8, :], places[2] * TILE, 1)


def stats_call(mine, theirs, extras, spots, places, dim):
    tiles = mine.shape[0]
    spec = pl.BlockSpec(
        (tiles, None, None, 4, TILE, 128), lambda b, *_: (0, b // 4, b % 4, 0, 0, 0)
    )
    return pl.pallas_call(
        functools.partial(stats_kernel, float(dim), spots),
        grid_spec=pltpu.PrefetchScalarGridSpec(
            num_scalar_prefetch=1,
            grid=(16,),
            in_specs=[spec] * 2 + [pl.BlockSpec(memory_space=pl.ANY)] * len(extras),
            out_specs=pl.BlockSpec((16, 8, 128), lambda b, *_: (0, 0, 0)),
            scratch_shapes=[
                pltpu.VMEM((4, 512, EXTRA), bf16),
                pltpu.SemaphoreType.DMA((len(extras),)),
            ],
        ),
        out_shape=jax.ShapeDtypeStruct((16, 8, 128), f32),
        cost_estimate=pl.CostEstimate(
            flops=10 * mine.size, bytes_accessed=8 * mine.size, transcendentals=mine.size
        ),
        compiler_params=pltpu.CompilerParams(
            dimension_semantics=("arbitrary",), vmem_limit_bytes=16 * 1024 * 1024
        ),
    )(places, mine, theirs, *extras)


def gain_kernel(half, head, gain, out):
    rows = head.shape[0]
    for r in range(0, rows, 128):
        column = jnp.broadcast_to(gain[0, :, r : r + 128], (128, 128)).T
        for t in range(out.shape[0]):
            tile = head[r : r + 128, t * 128 : t * 128 + 128].astype(f32) * column
            out[t, r : r + 128] = tile.astype(bf16)


def gain_call(head, norm_gain, half):
    depth, columns = head.shape[0] // 2, head.shape[1]
    rows = 512
    steps = depth // rows
    return pl.pallas_call(
        gain_kernel,
        grid_spec=pltpu.PrefetchScalarGridSpec(
            num_scalar_prefetch=1,
            grid=(steps,),
            in_specs=[
                pl.BlockSpec((rows, columns), lambda i, half: (half[0] * steps + i, 0)),
                pl.BlockSpec((1, 1, rows), lambda i, half: (half[0] * steps + i, 0, 0)),
            ],
            out_specs=pl.BlockSpec((columns // 128, rows, 128), lambda i, half: (0, i, 0)),
        ),
        out_shape=jax.ShapeDtypeStruct((columns // 128, depth, 128), bf16),
        cost_estimate=pl.CostEstimate(
            flops=2 * depth * columns, bytes_accessed=4 * depth * columns, transcendentals=0
        ),
        compiler_params=pltpu.CompilerParams(
            dimension_semantics=("arbitrary",), vmem_limit_bytes=16 * 1024 * 1024
        ),
    )(half.reshape(1).astype(jnp.int32), head, norm_gain.reshape(-1, 1, rows))


def rows_kernel(places, *refs):
    sources, out, sems = refs[:12], refs[12], refs[13]
    x = places[2]
    copies = []
    for k, source in enumerate(sources):
        jx, part = k // 3, k % 3
        start, width = PARTS[part]
        row = (jx % 4 * TILE, 0, jx % 2 * 128)[part]
        to = pl.multiple_of(lax.rem(x + jx, 4) * TILE, TILE)
        copies.append(
            pltpu.make_async_copy(
                source.at[pl.ds(row, TILE), pl.ds(0, width)],
                out.at[pl.ds(to, TILE), pl.ds(start, width)],
                sems.at[k],
            )
        )
    for copy in copies:
        copy.start()
    for copy in copies:
        copy.wait()


def rows_call(sources, places, cols):
    return pl.pallas_call(
        rows_kernel,
        grid_spec=pltpu.PrefetchScalarGridSpec(
            num_scalar_prefetch=1,
            grid=(1,),
            in_specs=[pl.BlockSpec(memory_space=pl.ANY)] * 12,
            out_specs=pl.BlockSpec((4 * TILE, cols), lambda i, places: (0, 0)),
            scratch_shapes=[pltpu.SemaphoreType.DMA((12,))],
        ),
        out_shape=jax.ShapeDtypeStruct((4 * TILE, cols), bf16),
        cost_estimate=pl.CostEstimate(
            flops=0, bytes_accessed=16 * TILE * cols, transcendentals=0
        ),
        compiler_params=pltpu.CompilerParams(vmem_limit_bytes=16 * 1024 * 1024),
    )(places, *sources)


def join_kernel(counts, *refs):
    total = sum(counts)
    at = 0
    for out, count in zip(refs[total:], counts):
        row = 0
        for piece in refs[at : at + count]:
            out[row : row + piece.shape[0]] = piece[...]
            row += piece.shape[0]
        at += count


def joined(groups):
    flat = [a for group in groups for a in group]
    return pl.pallas_call(
        functools.partial(join_kernel, [len(g) for g in groups]),
        out_shape=[
            jax.ShapeDtypeStruct((sum(a.shape[0] for a in g), g[0].shape[1]), g[0].dtype)
            for g in groups
        ],
        cost_estimate=pl.CostEstimate(
            flops=0, bytes_accessed=sum(4 * a.size for a in flat), transcendentals=0
        ),
        compiler_params=pltpu.CompilerParams(vmem_limit_bytes=16 * 1024 * 1024),
    )(*flat)


def combined(peaks, totals, picks):
    peak = jnp.max(peaks, axis=0)
    return peak, jnp.sum(totals * jnp.exp(peaks - peak), axis=0), jnp.sum(picks, axis=0)


def per_device(
    tokens,
    expert_hidden,
    routes,
    route_weight,
    expert_weight,
    norm_gain,
    head_weight,
    targets,
    rollout_logprob,
    advantages,
):
    x, y, z, h = (lax.axis_index(a) for a in (X, Y, Z, CORE))
    dim = tokens.shape[1]
    cols = dim // 2
    voc_dev = head_weight.shape[1]

    def beside(after):
        head, _ = lax.optimization_barrier((head_weight, after))
        sent = gain_call(head, norm_gain, 1 - h)
        return sent, gain_call(head, norm_gain, h)

    tile, (head_sent, head_mine) = experts_stage(
        tokens,
        expert_hidden,
        routes,
        route_weight,
        expert_weight,
        beside,
    )
    heads = (swap_cores(head_sent), head_mine)
    labels = lax.dynamic_slice_in_dim(targets, x * TILE, TILE, 0)
    extra = extra_columns(tile, labels)
    pieces = [tile[:, a : a + w] for a, w in PARTS]
    pieces[0] = jnp.concatenate([pieces[0], extra], axis=1)
    pieces = joined(
        [
            [p, moved(p, axes[0], -1), moved(p, axes[0], 2), moved(p, axes[0], 1)]
            for p, axes in zip(pieces, ORDERS)
        ]
    )
    seconds = [[moved(p, axes[1], k) for k in (-1, 2, 1)] for p, axes in zip(pieces, ORDERS)]
    own_a = joined([[p, second[0]] for p, second in zip(pieces, seconds)])
    own_b = joined([second[1:] for second in seconds])

    def sent(arrays, step):
        return [moved(p, axes[2], step) for p, axes in zip(arrays, ORDERS)]

    up_a, down_b = sent(own_a, -1), sent(own_b, 1)
    up_b, down_a = sent(own_b, -1), sent(own_a, 1)
    far_a, far_b = sent(up_a, -1), sent(down_b, 1)
    items, lhs = [], []
    for arrays, j3, j2 in (
        (own_a, 0, 0),
        (own_b, 0, 2),
        (up_a, 1, 0),
        (down_b, 3, 2),
        (up_b, 1, 2),
        (down_a, 3, 0),
        (far_a, 2, 0),
        (far_b, 2, 2),
    ):
        items += [(part, j3, j2) for part in range(3)]
        lhs += arrays
    places = jnp.stack([y, z, x, lax.axis_index(DP_VOCAB) * voc_dev]).astype(jnp.int32)
    sources = []
    for jx, near in enumerate((own_a, up_a, far_a, down_a)):
        sources += [own_a[0], near[1], (own_a, own_b)[jx // 2][2]]
    rows = rows_call(sources, places, cols)
    other = swap_cores(rows)
    group_layer = jnp.where(
        h == 0, jnp.concatenate([rows, other], axis=1), jnp.concatenate([other, rows], axis=1)
    )
    sums = head_call(items[:18], lhs[:18], heads, None)
    sums = head_call(items[18:], lhs[18:], heads, sums)
    spots = [(j3, 128 * j2) for _, j3, j2 in items[::3]]
    stats = stats_call(sums[1], swap_cores(sums[0]), lhs[::3], spots, places, dim)
    sent = lax.all_to_all(stats, DP, 0, 0, tiled=True)
    group = jnp.stack(combined(sent[:, 0], sent[:, 1], sent[:, 2]))
    sent = lax.all_gather(group, VOCAB, axis=0)
    peak, total, target_logit = combined(sent[:, 0], sent[:, 1], sent[:, 2])
    token_logprob = target_logit - (peak + jnp.log(total))
    token_loss = clipped_loss(token_logprob, rollout_logprob, advantages)

    return (group_layer, token_logprob, token_loss)


def solution(mesh):
    torus = Mesh(mesh.devices.reshape(4, 4, 4, 2), ("dp_0", "dp_1", "vocab_0", "vocab_1"))
    placed = (
        P(DP, None),
        P(DP, None, None),
        P(DP, None),
        P(DP, None),
        P(DP_VOCAB, None, None),
        P(),
        P(None, DP_VOCAB),
        P(DP),
        P(DP),
        P(DP),
    )
    return jax.shard_map(
        per_device,
        mesh=torus,
        in_specs=placed,
        out_specs=(P(DP, None), P(DP), P(DP)),
        check_vma=False,
    )
```

```python
import functools

import jax
import jax.numpy as jnp
from jax import lax
from jax.experimental import pallas as pl
from jax.experimental.pallas import tpu as pltpu
from jax.sharding import Mesh
from jax.sharding import PartitionSpec as P

X = "vocab_0"
Y = "dp_0"
Z = "dp_1"
CORE = "vocab_1"
VOCAB = ("vocab_0", "vocab_1")
DP_VOCAB = ("dp_0", "dp_1", "vocab_0", "vocab_1")
DP = ("dp_0", "dp_1")

norm_epsilon = 1e-06
clip_low = 0.8
clip_high = 1.2
dual_bound = 3.0
bf16 = jnp.bfloat16
f32 = jnp.float32

PARTS = ((0, 1152), (1152, 1152), (2304, 1280))
ORDERS = ((X, Y, Z), (Y, Z, X), (Z, X, Y))
EXTRA = 128
TILE = 32
FIRST_VMEM = 24 * 1024 * 1024
SECOND_VMEM = 19 * 1024 * 1024


def clipped_loss(logprob, rollout_logprob, advantages):
    ratio = jnp.exp(logprob - rollout_logprob)
    surrogate = jnp.minimum(ratio * advantages, jnp.clip(ratio, clip_low, clip_high) * advantages)
    bounded = jnp.where(
        advantages < 0.0, jnp.maximum(surrogate, dual_bound * advantages), surrogate
    )
    return -bounded


def dot(a, b):
    return jnp.dot(a, b, preferred_element_type=f32)


def moved(x, axis, step):
    n = lax.axis_size(axis)
    return lax.ppermute(x, axis, [(i, (i + step) % n) for i in range(n)])


def swap_cores(x):
    return lax.ppermute(x, CORE, [(0, 1), (1, 0)])


def bf16_terms(x):
    terms = []
    for _ in range(3):
        term = lax.reduce_precision(x, 8, 7)
        terms.append(term)
        x = x - term
    return terms


def experts_stage(tokens, expert_hidden, routes, route_weight, expert_weight, beside):
    x, h = lax.axis_index(X), lax.axis_index(CORE)
    rows, top = routes.shape
    width = expert_hidden.shape[2] // 2
    cols = tokens.shape[1] // 2
    blocks = rows // 16
    by_block = routes.reshape(blocks, 16 * top).T
    mine = (
        by_block[:, :, None] == (lax.iota(jnp.int32, 16) * 4 + x)[None, None, :]
    ).astype(bf16)
    n = 16 * top
    lower = (lax.iota(jnp.int32, n)[:, None] > lax.iota(jnp.int32, n)[None, :]).astype(bf16)
    before = dot(lower, mine.reshape(n, blocks * 16)).reshape(n, blocks, 16)
    slot = jnp.sum(before * mine.astype(f32), axis=2).astype(jnp.int32)
    place = (by_block // 4) * 24 + lax.iota(jnp.int32, blocks)[None, :] * 3 + slot
    place = jnp.where(by_block % 4 == x, place, -1).T.reshape(rows, top)
    select = (lax.iota(jnp.int32, 384)[:, None] == place.reshape(-1)[None, :]).astype(bf16)
    picked = dot(select, expert_hidden.reshape(rows * top, 2 * width)).astype(bf16)
    buffer = lax.dynamic_slice_in_dim(picked, h * width, width, 1).reshape(16, 24, width)
    own = lax.all_to_all(buffer, DP, 0, 0, tiled=True).reshape(384, width)
    other = swap_cores(own)
    weight = expert_weight[0]
    weight_own = lax.dynamic_slice_in_dim(weight, h * cols, cols, 1)
    weight_other = lax.dynamic_slice_in_dim(swap_cores(weight), h * cols, cols, 1)
    product = (dot(own, weight_own) + dot(other, weight_other)).astype(bf16)
    back = lax.all_to_all(product.reshape(16, 24, cols), DP, 0, 0, tiled=True)
    back, beside = lax.optimization_barrier((back, beside(product)))
    gate = jnp.sum(
        jnp.where(
            place[:, :, None] == lax.iota(jnp.int32, 384)[None, None, :],
            route_weight[:, :, None],
            0.0,
        ),
        axis=1,
    )
    high, low, _ = bf16_terms(gate)
    both = dot(jnp.concatenate([high, low]).astype(bf16), back.reshape(384, cols))
    partial = (both[:rows] + both[rows:]).astype(bf16)
    parts = lax.all_to_all(partial.reshape(4, rows // 4, cols), X, 0, 0, tiled=True)
    moe = jnp.sum(parts.astype(f32), axis=0)
    mine_tokens = lax.dynamic_slice(tokens, (x * TILE, h * cols), (TILE, cols))
    return (mine_tokens.astype(f32) + moe).astype(bf16), beside


def extra_columns(tile, labels):
    wide = tile.astype(f32)
    squares = jnp.sum(wide * wide, axis=1)
    lanes = bf16_terms(squares + swap_cores(squares))
    lanes += [((labels // 128**k) % 128).astype(f32) for k in range(3)]
    lane = lax.broadcasted_iota(jnp.int32, (TILE, EXTRA), 1)
    out = jnp.zeros((TILE, EXTRA), f32)
    for k, value in enumerate(lanes):
        out = jnp.where(lane == k, value[:, None], out)
    return out.astype(bf16)


def rows_of(part, j3, j2, j1):
    if part == 0:
        return j2, j3, j1
    if part == 1:
        return j1, j2, j3
    return j3, j1, j2


def head_kernel(items, first, places, *refs):
    count = len(items)
    lhs, (head_theirs, head_mine) = refs[:count], refs[count : count + 2]
    before, after = refs[count + 2 : -4], refs[-4:]
    sums, (extra, layer) = after[:2], after[2:]
    n = pl.program_id(0)
    for k in range(2):
        sums[k][...] = jnp.zeros_like(sums[k]) if first else before[k][...]
    for k, (part, j3, j2_first) in enumerate(items):
        start, width = PARTS[part]
        rhs = jnp.concatenate(
            [head_theirs[0, start : start + width], head_mine[0, start : start + width]], axis=1
        )
        result = dot(lhs[k][:, :width], rhs)
        for b in range(8):
            jy, jz, jx = rows_of(part, j3, j2_first + b // 4, b % 4)
            rows = slice(b * TILE, (b + 1) * TILE)
            for side in range(2):
                sums[side][0, jy, jz, jx] += result[rows, side * 128 : side * 128 + 128]

    @pl.when(n == 0)
    def _():
        if not first:
            extra[...] = before[2][...]
            layer[...] = before[3][...]
        for k, (part, j3, j2_first) in enumerate(items):
            start, width = PARTS[part]
            if part == 0:
                extra[j3, j2_first * 128 : j2_first * 128 + 256] = lhs[k][:, width:]
            for b in range(8):
                jy, jz, jx = rows_of(part, j3, j2_first + b // 4, b % 4)
                if jy == 0 and jz == 0:
                    to = pl.multiple_of(lax.rem(places[2] + jx, 4) * TILE, TILE)
                    layer[pl.ds(to, TILE), start : start + width] = lhs[k][
                        b * TILE : (b + 1) * TILE, :width
                    ]


def in_vmem(x):
    return pltpu.with_memory_space_constraint(x, pltpu.MemorySpace.VMEM)


def in_hbm(x):
    return pltpu.with_memory_space_constraint(x, pltpu.MemorySpace.HBM)


def head_call(items, lhs, heads, places, before):
    tiles, depth, _ = heads[0].shape
    whole = pl.BlockSpec(memory_space=pltpu.MemorySpace.VMEM)
    head_spec = pl.BlockSpec((1, depth, 128), lambda n, *_: (n, 0, 0))
    sum_spec = pl.BlockSpec((1, 4, 4, 4, TILE, 128), lambda n, *_: (n, 0, 0, 0, 0, 0))
    sum_shape = pltpu.HBM((tiles, 4, 4, 4, TILE, 128), f32)
    after_specs = [sum_spec] * 2 + [
        pl.BlockSpec((4, 512, EXTRA), lambda n, *_: (0, 0, 0)),
        pl.BlockSpec((4 * TILE, depth), lambda n, *_: (0, 0)),
    ]
    size = sum(a.size for a in lhs)
    return pl.pallas_call(
        functools.partial(head_kernel, items, not before),
        grid_spec=pltpu.PrefetchScalarGridSpec(
            num_scalar_prefetch=1,
            grid=(tiles,),
            in_specs=[whole] * len(lhs) + [head_spec] * 2 + after_specs[: len(before)],
            out_specs=after_specs,
        ),
        out_shape=[
            sum_shape,
            sum_shape,
            jax.ShapeDtypeStruct((4, 512, EXTRA), bf16),
            jax.ShapeDtypeStruct((4 * TILE, depth), bf16),
        ],
        cost_estimate=pl.CostEstimate(
            flops=2 * size * tiles * 256, bytes_accessed=2 * size, transcendentals=0
        ),
        compiler_params=pltpu.CompilerParams(
            dimension_semantics=("arbitrary",), vmem_limit_bytes=(SECOND_VMEM if before else FIRST_VMEM)
        ),
    )(
        places,
        *[in_vmem(a) for a in lhs],
        *[in_hbm(a) for a in heads],
        *[in_hbm(a) for a in before[:2]],
        *before[2:],
    )


def stats_kernel(dim, places, mine, theirs, extra, out):
    jy = pl.program_id(0)
    row = lax.broadcasted_iota(jnp.int32, (EXTRA, 256), 0)
    left = lax.broadcasted_iota(jnp.int32, (EXTRA, 256), 1) < 128
    digits = jnp.where(row == 3, 1.0, jnp.where(row == 4, 128.0, 16384.0))
    digits = jnp.where((row >= 3) & (row < 6), digits, 0.0)
    spreader = jnp.where(left, jnp.where(row < 3, 1.0, 0.0), digits).astype(bf16)
    lane = lax.broadcasted_iota(jnp.int32, (128, 128), 1)
    sub = lax.broadcasted_iota(jnp.int32, (8, 128), 0)
    for jz in range(4):
        spread = dot(extra[jz, pl.ds(pl.multiple_of(jy * 128, 128), 128), :], spreader)
        scale = lax.rsqrt(spread[:, :128] / dim + norm_epsilon)
        wanted = spread[:, 128:].astype(jnp.int32) - places[3] - lane
        tiles = [
            (mine[t, jz].reshape(128, 128) + theirs[t, jz].reshape(128, 128)) * scale
            for t in range(theirs.shape[0])
        ]
        peak = functools.reduce(jnp.maximum, tiles)
        total = functools.reduce(jnp.add, [jnp.exp(v - peak) for v in tiles])
        pick = functools.reduce(
            jnp.add, [jnp.where(wanted == 128 * t, v, 0.0) for t, v in enumerate(tiles)]
        )
        peak, total, pick = peak.T, total.T, pick.T
        row_peak = jnp.max(peak, axis=0, keepdims=True)
        row_total = jnp.sum(total * jnp.exp(peak - row_peak), axis=0, keepdims=True)
        row_pick = jnp.sum(pick, axis=0, keepdims=True)
        three = jnp.where(sub == 0, row_peak, jnp.where(sub == 1, row_total, row_pick))
        group = lax.rem(places[0] + jy, 4) * 4 + lax.rem(places[1] + jz, 4)
        out[group] = pltpu.roll(three, places[2] * TILE, 1)


def stats_call(mine, theirs, extra, places, dim):
    block = pl.BlockSpec(
        (mine.shape[0], None, 4, 4, TILE, 128), lambda b, *_: (0, b, 0, 0, 0, 0)
    )
    size = mine.size
    return pl.pallas_call(
        functools.partial(stats_kernel, float(dim)),
        grid_spec=pltpu.PrefetchScalarGridSpec(
            num_scalar_prefetch=1,
            grid=(4,),
            in_specs=[block] * 2 + [pl.BlockSpec((4, 512, EXTRA), lambda b, *_: (0, 0, 0))],
            out_specs=pl.BlockSpec((16, 8, 128), lambda b, *_: (0, 0, 0)),
        ),
        out_shape=jax.ShapeDtypeStruct((16, 8, 128), f32),
        cost_estimate=pl.CostEstimate(
            flops=10 * size, bytes_accessed=8 * size, transcendentals=size
        ),
        compiler_params=pltpu.CompilerParams(
            dimension_semantics=("arbitrary",), vmem_limit_bytes=16 * 1024 * 1024
        ),
    )(places, in_hbm(mine), in_hbm(theirs), extra)


def gain_kernel(half, head, gain, out):
    rows = head.shape[0]
    for r in range(0, rows, 128):
        column = jnp.broadcast_to(gain[0, :, r : r + 128], (128, 128)).T
        for t in range(out.shape[0]):
            tile = head[r : r + 128, t * 128 : t * 128 + 128].astype(f32) * column
            out[t, r : r + 128] = tile.astype(bf16)


def gain_call(head, norm_gain, half):
    depth, columns = head.shape[0] // 2, head.shape[1]
    rows = 512
    steps = depth // rows
    return pl.pallas_call(
        gain_kernel,
        grid_spec=pltpu.PrefetchScalarGridSpec(
            num_scalar_prefetch=1,
            grid=(steps,),
            in_specs=[
                pl.BlockSpec((rows, columns), lambda i, half: (half[0] * steps + i, 0)),
                pl.BlockSpec((1, 1, rows), lambda i, half: (half[0] * steps + i, 0, 0)),
            ],
            out_specs=pl.BlockSpec((columns // 128, rows, 128), lambda i, half: (0, i, 0)),
        ),
        out_shape=jax.ShapeDtypeStruct((columns // 128, depth, 128), bf16),
        cost_estimate=pl.CostEstimate(
            flops=2 * depth * columns, bytes_accessed=4 * depth * columns, transcendentals=0
        ),
        compiler_params=pltpu.CompilerParams(
            dimension_semantics=("arbitrary",), vmem_limit_bytes=16 * 1024 * 1024
        ),
    )(half.reshape(1).astype(jnp.int32), head, norm_gain.reshape(-1, 1, rows))


def join_kernel(counts, *refs):
    total = sum(counts)
    at = 0
    for out, count in zip(refs[total:], counts):
        row = 0
        for piece in refs[at : at + count]:
            out[row : row + piece.shape[0]] = piece[...]
            row += piece.shape[0]
        at += count


def joined(groups):
    flat = [a for group in groups for a in group]
    return pl.pallas_call(
        functools.partial(join_kernel, [len(g) for g in groups]),
        out_shape=[
            jax.ShapeDtypeStruct((sum(a.shape[0] for a in g), g[0].shape[1]), g[0].dtype)
            for g in groups
        ],
        cost_estimate=pl.CostEstimate(
            flops=0, bytes_accessed=sum(4 * a.size for a in flat), transcendentals=0
        ),
        compiler_params=pltpu.CompilerParams(vmem_limit_bytes=16 * 1024 * 1024),
    )(*flat)


def combined(peaks, totals, picks):
    peak = jnp.max(peaks, axis=0)
    return peak, jnp.sum(totals * jnp.exp(peaks - peak), axis=0), jnp.sum(picks, axis=0)


def per_device(
    tokens,
    expert_hidden,
    routes,
    route_weight,
    expert_weight,
    norm_gain,
    head_weight,
    targets,
    rollout_logprob,
    advantages,
):
    x, y, z, h = (lax.axis_index(a) for a in (X, Y, Z, CORE))
    dim = tokens.shape[1]
    cols = dim // 2
    voc_dev = head_weight.shape[1]

    def beside(after):
        head, _ = lax.optimization_barrier((head_weight, after))
        sent = gain_call(head, norm_gain, 1 - h)
        return sent, gain_call(head, norm_gain, h)

    tile, (head_sent, head_mine) = experts_stage(
        tokens,
        expert_hidden,
        routes,
        route_weight,
        expert_weight,
        beside,
    )
    heads = (swap_cores(head_sent), head_mine)
    labels = lax.dynamic_slice_in_dim(targets, x * TILE, TILE, 0)
    extra = extra_columns(tile, labels)
    pieces = [tile[:, a : a + w] for a, w in PARTS]
    pieces[0] = jnp.concatenate([pieces[0], extra], axis=1)
    pieces = joined(
        [
            [p, moved(p, axes[0], -1), moved(p, axes[0], 2), moved(p, axes[0], 1)]
            for p, axes in zip(pieces, ORDERS)
        ]
    )
    seconds = [[moved(p, axes[1], k) for k in (-1, 2, 1)] for p, axes in zip(pieces, ORDERS)]
    own_a = joined([[p, second[0]] for p, second in zip(pieces, seconds)])
    own_b = joined([second[1:] for second in seconds])

    def sent(arrays, step):
        return [moved(p, axes[2], step) for p, axes in zip(arrays, ORDERS)]

    up_a, down_b = sent(own_a, -1), sent(own_b, 1)
    up_b, down_a = sent(own_b, -1), sent(own_a, 1)
    far_a, far_b = sent(up_a, -1), sent(down_b, 1)
    items, lhs = [], []
    for arrays, j3, j2 in (
        (own_a, 0, 0),
        (own_b, 0, 2),
        (up_a, 1, 0),
        (down_b, 3, 2),
        (up_b, 1, 2),
        (down_a, 3, 0),
        (far_a, 2, 0),
        (far_b, 2, 2),
    ):
        items += [(part, j3, j2) for part in range(3)]
        lhs += arrays
    places = jnp.stack([y, z, x, lax.axis_index(DP_VOCAB) * voc_dev]).astype(jnp.int32)
    before = head_call(items[:18], lhs[:18], heads, places, ())
    theirs, mine, extra, rows = head_call(items[18:], lhs[18:], heads, places, before)
    stats = stats_call(mine, swap_cores(theirs), extra, places, dim)
    other = swap_cores(rows)
    group_layer = jnp.where(
        h == 0, jnp.concatenate([rows, other], axis=1), jnp.concatenate([other, rows], axis=1)
    )
    sent = lax.all_to_all(stats, DP, 0, 0, tiled=True)
    group = jnp.stack(combined(sent[:, 0], sent[:, 1], sent[:, 2]))
    sent = lax.all_gather(group, VOCAB, axis=0)
    peak, total, target_logit = combined(sent[:, 0], sent[:, 1], sent[:, 2])
    token_logprob = target_logit - (peak + jnp.log(total))
    token_loss = clipped_loss(token_logprob, rollout_logprob, advantages)

    return (group_layer, token_logprob, token_loss)


def solution(mesh):
    torus = Mesh(mesh.devices.reshape(4, 4, 4, 2), ("dp_0", "dp_1", "vocab_0", "vocab_1"))
    placed = (
        P(DP, None),
        P(DP, None, None),
        P(DP, None),
        P(DP, None),
        P(DP_VOCAB, None, None),
        P(),
        P(None, DP_VOCAB),
        P(DP),
        P(DP),
        P(DP),
    )
    return jax.shard_map(
        per_device,
        mesh=torus,
        in_specs=placed,
        out_specs=(P(DP, None), P(DP), P(DP)),
        check_vma=False,
    )
```

```python
import functools

import jax
import jax.numpy as jnp
from jax import lax
from jax.experimental import pallas as pl
from jax.experimental.pallas import tpu as pltpu
from jax.sharding import Mesh
from jax.sharding import PartitionSpec as P

X = "vocab_0"
Y = "dp_0"
Z = "dp_1"
CORE = "vocab_1"
VOCAB = ("vocab_0", "vocab_1")
DP_VOCAB = ("dp_0", "dp_1", "vocab_0", "vocab_1")
DP = ("dp_0", "dp_1")

norm_epsilon = 1e-06
clip_low = 0.8
clip_high = 1.2
dual_bound = 3.0
bf16 = jnp.bfloat16
f32 = jnp.float32

PARTS = ((0, 1152), (1152, 1152), (2304, 1280))
ORDERS = ((X, Y, Z), (Y, Z, X), (Z, X, Y))
EXTRA = 128
TILE = 32
FIRST_VMEM = 24 * 1024 * 1024
SECOND_VMEM = 19 * 1024 * 1024


def clipped_loss(logprob, rollout_logprob, advantages):
    ratio = jnp.exp(logprob - rollout_logprob)
    surrogate = jnp.minimum(ratio * advantages, jnp.clip(ratio, clip_low, clip_high) * advantages)
    bounded = jnp.where(
        advantages < 0.0, jnp.maximum(surrogate, dual_bound * advantages), surrogate
    )
    return -bounded


def dot(a, b):
    return jnp.dot(a, b, preferred_element_type=f32)


def moved(x, axis, step):
    n = lax.axis_size(axis)
    return lax.ppermute(x, axis, [(i, (i + step) % n) for i in range(n)])


def swap_cores(x):
    return lax.ppermute(x, CORE, [(0, 1), (1, 0)])


def bf16_terms(x):
    terms = []
    for _ in range(3):
        term = lax.reduce_precision(x, 8, 7)
        terms.append(term)
        x = x - term
    return terms


def expert_kernel(half, own, other, weight_own, weight_other, out):
    out[...] = (dot(own[...], weight_own[...]) + dot(other[...], weight_other[...])).astype(bf16)


def expert_call(own, other, weight_own, weight_other, half, chunk):
    rows, depth = own.shape
    cols, block = weight_own.shape[1] // 4, 896
    steps = cols // block
    rows_spec = pl.BlockSpec((rows, depth), lambda n, half: (0, 0))
    weight_spec = pl.BlockSpec(
        (depth, block), lambda n, half: (0, (2 * half[0] + chunk) * steps + n)
    )
    return pl.pallas_call(
        expert_kernel,
        grid_spec=pltpu.PrefetchScalarGridSpec(
            num_scalar_prefetch=1,
            grid=(steps,),
            in_specs=[rows_spec] * 2 + [weight_spec] * 2,
            out_specs=pl.BlockSpec((rows, block), lambda n, half: (0, n)),
        ),
        out_shape=jax.ShapeDtypeStruct((rows, cols), bf16),
        cost_estimate=pl.CostEstimate(
            flops=4 * rows * depth * cols, bytes_accessed=4 * depth * cols, transcendentals=0
        ),
        compiler_params=pltpu.CompilerParams(
            dimension_semantics=("arbitrary",), vmem_limit_bytes=16 * 1024 * 1024
        ),
    )(half.reshape(1).astype(jnp.int32), own, other, weight_own, weight_other)


def experts_stage(tokens, expert_hidden, routes, route_weight, expert_weight, beside):
    x, h = lax.axis_index(X), lax.axis_index(CORE)
    rows, top = routes.shape
    width = expert_hidden.shape[2] // 2
    cols = tokens.shape[1] // 2
    blocks = rows // 16
    by_block = routes.reshape(blocks, 16 * top).T
    mine = (
        by_block[:, :, None] == (lax.iota(jnp.int32, 16) * 4 + x)[None, None, :]
    ).astype(bf16)
    n = 16 * top
    lower = (lax.iota(jnp.int32, n)[:, None] > lax.iota(jnp.int32, n)[None, :]).astype(bf16)
    before = dot(lower, mine.reshape(n, blocks * 16)).reshape(n, blocks, 16)
    slot = jnp.sum(before * mine.astype(f32), axis=2).astype(jnp.int32)
    place = (by_block // 4) * 24 + lax.iota(jnp.int32, blocks)[None, :] * 3 + slot
    place = jnp.where(by_block % 4 == x, place, -1).T.reshape(rows, top)
    select = (lax.iota(jnp.int32, 384)[:, None] == place.reshape(-1)[None, :]).astype(bf16)
    picked = dot(select, expert_hidden.reshape(rows * top, 2 * width)).astype(bf16)
    buffer = lax.dynamic_slice_in_dim(picked, h * width, width, 1).reshape(16, 24, width)
    own = lax.all_to_all(buffer, DP, 0, 0, tiled=True).reshape(384, width)
    other = swap_cores(own)
    weight = expert_weight[0]
    weight_other = swap_cores(weight)
    products = [expert_call(own, other, weight, weight_other, h, c) for c in range(2)]
    backs = [
        lax.all_to_all(p.reshape(16, 24, cols // 2), DP, 0, 0, tiled=True) for p in products
    ]
    backs[0], products[1] = lax.optimization_barrier((backs[0], products[1]))
    backs[1], beside = lax.optimization_barrier((backs[1], beside(products[1])))
    gate = jnp.sum(
        jnp.where(
            place[:, :, None] == lax.iota(jnp.int32, 384)[None, None, :],
            route_weight[:, :, None],
            0.0,
        ),
        axis=1,
    )
    high, low, _ = bf16_terms(gate)
    gates = jnp.concatenate([high, low]).astype(bf16)
    moe = []
    for back in backs:
        both = dot(gates, back.reshape(384, cols // 2))
        partial = (both[:rows] + both[rows:]).astype(bf16)
        quarters = [
            lax.dynamic_slice_in_dim(partial, (x + k) % 4 * TILE, TILE, 0) for k in range(4)
        ]
        arrived = [quarters[0]] + [moved(quarters[k], X, k) for k in (2, 1, 3)]
        moe.append(functools.reduce(jnp.add, [q.astype(f32) for q in arrived]))
    moe = jnp.concatenate(moe, axis=1)
    mine_tokens = lax.dynamic_slice(tokens, (x * TILE, h * cols), (TILE, cols))
    return (mine_tokens.astype(f32) + moe).astype(bf16), beside


def extra_columns(tile, labels):
    wide = tile.astype(f32)
    squares = jnp.sum(wide * wide, axis=1)
    lanes = bf16_terms(squares + swap_cores(squares))
    lanes += [((labels // 128**k) % 128).astype(f32) for k in range(3)]
    lane = lax.broadcasted_iota(jnp.int32, (TILE, EXTRA), 1)
    out = jnp.zeros((TILE, EXTRA), f32)
    for k, value in enumerate(lanes):
        out = jnp.where(lane == k, value[:, None], out)
    return out.astype(bf16)


def rows_of(part, j3, j2, j1):
    if part == 0:
        return j2, j3, j1
    if part == 1:
        return j1, j2, j3
    return j3, j1, j2


def head_kernel(items, sides, first, with_rows, *refs):
    count = len(items)
    lhs, heads, rest = refs[:count], refs[count : count + sides], refs[count + sides :]
    places, rest = rest[0], rest[1:]
    outs = sides + (2 if with_rows else 0)
    before, after = rest[:-outs], rest[-outs:]
    sums = after[:sides]
    n = pl.program_id(0)
    for k in range(sides):
        sums[k][...] = jnp.zeros_like(sums[k]) if first else before[k][...]
    for k, (part, j3, j2_first) in enumerate(items):
        start, width = PARTS[part]
        rhs = jnp.concatenate([head[0, start : start + width] for head in heads], axis=1)
        result = dot(lhs[k][:, :width], rhs)
        for b in range(8):
            jy, jz, jx = rows_of(part, j3, j2_first + b // 4, b % 4)
            rows = slice(b * TILE, (b + 1) * TILE)
            for side in range(sides):
                sums[side][0, jy, jz, jx] += result[rows, side * 128 : side * 128 + 128]
    if not with_rows:
        return
    extra, layer = after[sides:]

    @pl.when(n == 0)
    def _():
        if not first:
            extra[...] = before[sides][...]
            layer[...] = before[sides + 1][...]
        for k, (part, j3, j2_first) in enumerate(items):
            start, width = PARTS[part]
            if part == 0:
                extra[j3, j2_first * 128 : j2_first * 128 + 256] = lhs[k][:, width:]
            for b in range(8):
                jy, jz, jx = rows_of(part, j3, j2_first + b // 4, b % 4)
                if jy == 0 and jz == 0:
                    to = pl.multiple_of(lax.rem(places[2] + jx, 4) * TILE, TILE)
                    layer[pl.ds(to, TILE), start : start + width] = lhs[k][
                        b * TILE : (b + 1) * TILE, :width
                    ]


def in_vmem(x):
    return pltpu.with_memory_space_constraint(x, pltpu.MemorySpace.VMEM)


def in_hbm(x):
    return pltpu.with_memory_space_constraint(x, pltpu.MemorySpace.HBM)


def head_call(items, lhs, heads, places, before, with_rows):
    tiles, depth, _ = heads[0].shape
    sides = len(heads)
    whole = pl.BlockSpec(memory_space=pltpu.MemorySpace.VMEM)
    head_spec = pl.BlockSpec((1, depth, 128), lambda n: (n, 0, 0))
    sum_spec = pl.BlockSpec((1, 4, 4, 4, TILE, 128), lambda n: (n, 0, 0, 0, 0, 0))
    after_specs = [sum_spec] * sides
    after_shape = [pltpu.HBM((tiles, 4, 4, 4, TILE, 128), f32)] * sides
    if with_rows:
        after_specs += [
            pl.BlockSpec((4, 512, EXTRA), lambda n: (0, 0, 0)),
            pl.BlockSpec((4 * TILE, depth), lambda n: (0, 0)),
        ]
        after_shape += [
            jax.ShapeDtypeStruct((4, 512, EXTRA), bf16),
            jax.ShapeDtypeStruct((4 * TILE, depth), bf16),
        ]
    size = sum(a.size for a in lhs)
    return pl.pallas_call(
        functools.partial(head_kernel, items, sides, not before, with_rows),
        grid=(tiles,),
        in_specs=[
            *[whole] * len(lhs),
            *[head_spec] * sides,
            pl.BlockSpec(memory_space=pltpu.MemorySpace.SMEM),
            *after_specs[: len(before)],
        ],
        out_specs=after_specs,
        out_shape=after_shape,
        cost_estimate=pl.CostEstimate(
            flops=2 * size * tiles * 128 * sides, bytes_accessed=2 * size, transcendentals=0
        ),
        compiler_params=pltpu.CompilerParams(
            dimension_semantics=("arbitrary",),
            vmem_limit_bytes=SECOND_VMEM if before else FIRST_VMEM,
        ),
    )(
        *[in_vmem(a) for a in lhs],
        *[in_hbm(a) for a in heads],
        places,
        *[in_hbm(a) for a in before[:sides]],
        *before[sides:],
    )


def stats_kernel(dim, places, mine, theirs, extra, out):
    jy = pl.program_id(0)
    row = lax.broadcasted_iota(jnp.int32, (EXTRA, 256), 0)
    left = lax.broadcasted_iota(jnp.int32, (EXTRA, 256), 1) < 128
    digits = jnp.where(row == 3, 1.0, jnp.where(row == 4, 128.0, 16384.0))
    digits = jnp.where((row >= 3) & (row < 6), digits, 0.0)
    spreader = jnp.where(left, jnp.where(row < 3, 1.0, 0.0), digits).astype(bf16)
    lane = lax.broadcasted_iota(jnp.int32, (128, 128), 1)
    sub = lax.broadcasted_iota(jnp.int32, (8, 128), 0)
    for jz in range(4):
        spread = dot(extra[jz, pl.ds(pl.multiple_of(jy * 128, 128), 128), :], spreader)
        scale = lax.rsqrt(spread[:, :128] / dim + norm_epsilon)
        wanted = spread[:, 128:].astype(jnp.int32) - places[3] - lane
        tiles = [
            (mine[t, jz].reshape(128, 128) + theirs[t, jz].reshape(128, 128)) * scale
            for t in range(theirs.shape[0])
        ]
        peak = functools.reduce(jnp.maximum, tiles)
        total = functools.reduce(jnp.add, [jnp.exp(v - peak) for v in tiles])
        pick = functools.reduce(
            jnp.add, [jnp.where(wanted == 128 * t, v, 0.0) for t, v in enumerate(tiles)]
        )
        peak, total, pick = peak.T, total.T, pick.T
        row_peak = jnp.max(peak, axis=0, keepdims=True)
        row_total = jnp.sum(total * jnp.exp(peak - row_peak), axis=0, keepdims=True)
        row_pick = jnp.sum(pick, axis=0, keepdims=True)
        three = jnp.where(sub == 0, row_peak, jnp.where(sub == 1, row_total, row_pick))
        group = lax.rem(places[0] + jy, 4) * 4 + lax.rem(places[1] + jz, 4)
        out[group] = pltpu.roll(three, places[2] * TILE, 1)


def stats_call(mine, theirs, extra, places, dim):
    block = pl.BlockSpec(
        (mine.shape[0], None, 4, 4, TILE, 128), lambda b, *_: (0, b, 0, 0, 0, 0)
    )
    size = mine.size
    return pl.pallas_call(
        functools.partial(stats_kernel, float(dim)),
        grid_spec=pltpu.PrefetchScalarGridSpec(
            num_scalar_prefetch=1,
            grid=(4,),
            in_specs=[block] * 2 + [pl.BlockSpec((4, 512, EXTRA), lambda b, *_: (0, 0, 0))],
            out_specs=pl.BlockSpec((16, 8, 128), lambda b, *_: (0, 0, 0)),
        ),
        out_shape=jax.ShapeDtypeStruct((16, 8, 128), f32),
        cost_estimate=pl.CostEstimate(
            flops=10 * size, bytes_accessed=8 * size, transcendentals=size
        ),
        compiler_params=pltpu.CompilerParams(
            dimension_semantics=("arbitrary",), vmem_limit_bytes=16 * 1024 * 1024
        ),
    )(places, in_hbm(mine), in_hbm(theirs), extra)


def gain_kernel(half, head, gain, out):
    rows = head.shape[0]
    for r in range(0, rows, 128):
        column = jnp.broadcast_to(gain[0, :, r : r + 128], (128, 128)).T
        for t in range(out.shape[0]):
            tile = head[r : r + 128, t * 128 : t * 128 + 128].astype(f32) * column
            out[t, r : r + 128] = tile.astype(bf16)


def gain_call(head, norm_gain, half):
    depth, columns = head.shape[0] // 2, head.shape[1]
    rows = 512
    steps = depth // rows
    return pl.pallas_call(
        gain_kernel,
        grid_spec=pltpu.PrefetchScalarGridSpec(
            num_scalar_prefetch=1,
            grid=(steps,),
            in_specs=[
                pl.BlockSpec((rows, columns), lambda i, half: (half[0] * steps + i, 0)),
                pl.BlockSpec((1, 1, rows), lambda i, half: (half[0] * steps + i, 0, 0)),
            ],
            out_specs=pl.BlockSpec((columns // 128, rows, 128), lambda i, half: (0, i, 0)),
        ),
        out_shape=jax.ShapeDtypeStruct((columns // 128, depth, 128), bf16),
        cost_estimate=pl.CostEstimate(
            flops=2 * depth * columns, bytes_accessed=4 * depth * columns, transcendentals=0
        ),
        compiler_params=pltpu.CompilerParams(
            dimension_semantics=("arbitrary",), vmem_limit_bytes=16 * 1024 * 1024
        ),
    )(half.reshape(1).astype(jnp.int32), head, norm_gain.reshape(-1, 1, rows))


def join_kernel(counts, *refs):
    total = sum(counts)
    at = 0
    for out, count in zip(refs[total:], counts):
        row = 0
        for piece in refs[at : at + count]:
            out[row : row + piece.shape[0]] = piece[...]
            row += piece.shape[0]
        at += count


def joined(groups):
    flat = [a for group in groups for a in group]
    return pl.pallas_call(
        functools.partial(join_kernel, [len(g) for g in groups]),
        out_shape=[
            jax.ShapeDtypeStruct((sum(a.shape[0] for a in g), g[0].shape[1]), g[0].dtype)
            for g in groups
        ],
        cost_estimate=pl.CostEstimate(
            flops=0, bytes_accessed=sum(4 * a.size for a in flat), transcendentals=0
        ),
        compiler_params=pltpu.CompilerParams(vmem_limit_bytes=16 * 1024 * 1024),
    )(*flat)


def combined(peaks, totals, picks):
    peak = jnp.max(peaks, axis=0)
    return peak, jnp.sum(totals * jnp.exp(peaks - peak), axis=0), jnp.sum(picks, axis=0)


def per_device(
    tokens,
    expert_hidden,
    routes,
    route_weight,
    expert_weight,
    norm_gain,
    head_weight,
    targets,
    rollout_logprob,
    advantages,
):
    x, y, z, h = (lax.axis_index(a) for a in (X, Y, Z, CORE))
    dim = tokens.shape[1]
    cols = dim // 2
    voc_dev = head_weight.shape[1]

    def beside(after):
        head, _ = lax.optimization_barrier((head_weight, after))
        sent = gain_call(head, norm_gain, 1 - h)
        return sent, gain_call(head, norm_gain, h)

    tile, (head_sent, head_mine) = experts_stage(
        tokens,
        expert_hidden,
        routes,
        route_weight,
        expert_weight,
        beside,
    )
    heads = (swap_cores(head_sent), head_mine)
    labels = lax.dynamic_slice_in_dim(targets, x * TILE, TILE, 0)
    extra = extra_columns(tile, labels)
    pieces = [tile[:, a : a + w] for a, w in PARTS]
    pieces[0] = jnp.concatenate([pieces[0], extra], axis=1)
    pieces = joined(
        [
            [p, moved(p, axes[0], -1), moved(p, axes[0], 2), moved(p, axes[0], 1)]
            for p, axes in zip(pieces, ORDERS)
        ]
    )
    seconds = [[moved(p, axes[1], k) for k in (-1, 2, 1)] for p, axes in zip(pieces, ORDERS)]
    own_a = joined([[p, second[0]] for p, second in zip(pieces, seconds)])
    own_b = joined([second[1:] for second in seconds])

    def sent(arrays, step):
        return [moved(p, axes[2], step) for p, axes in zip(arrays, ORDERS)]

    up_a, down_b = sent(own_a, -1), sent(own_b, 1)
    up_b, down_a = sent(own_b, -1), sent(own_a, 1)
    far_a, far_b = sent(up_a, -1), sent(down_b, 1)
    items, lhs = [], []
    for arrays, j3, j2 in (
        (own_a, 0, 0),
        (own_b, 0, 2),
        (up_a, 1, 0),
        (down_b, 3, 2),
        (up_b, 1, 2),
        (down_a, 3, 0),
        (far_a, 2, 0),
        (far_b, 2, 2),
    ):
        items += [(part, j3, j2) for part in range(3)]
        lhs += arrays
    places = jnp.stack([y, z, x, lax.axis_index(DP_VOCAB) * voc_dev]).astype(jnp.int32)
    theirs, mine, extra, rows = head_call(items[:18], lhs[:18], heads, places, (), True)
    (theirs,) = head_call(items[18:], lhs[18:], heads[:1], places, (theirs,), False)
    theirs, mine, lhs[18:] = lax.optimization_barrier((theirs, mine, lhs[18:]))
    theirs = swap_cores(theirs)
    mine, extra, rows = head_call(
        items[18:], lhs[18:], heads[1:], places, (mine, extra, rows), True
    )
    stats = stats_call(mine, theirs, extra, places, dim)
    other = swap_cores(rows)
    group_layer = jnp.where(
        h == 0, jnp.concatenate([rows, other], axis=1), jnp.concatenate([other, rows], axis=1)
    )
    sent = lax.all_to_all(stats, DP, 0, 0, tiled=True)
    group = jnp.stack(combined(sent[:, 0], sent[:, 1], sent[:, 2]))
    sent = lax.all_gather(group, VOCAB, axis=0)
    peak, total, target_logit = combined(sent[:, 0], sent[:, 1], sent[:, 2])
    token_logprob = target_logit - (peak + jnp.log(total))
    token_loss = clipped_loss(token_logprob, rollout_logprob, advantages)

    return (group_layer, token_logprob, token_loss)


def solution(mesh):
    torus = Mesh(mesh.devices.reshape(4, 4, 4, 2), ("dp_0", "dp_1", "vocab_0", "vocab_1"))
    placed = (
        P(DP, None),
        P(DP, None, None),
        P(DP, None),
        P(DP, None),
        P(DP_VOCAB, None, None),
        P(),
        P(None, DP_VOCAB),
        P(DP),
        P(DP),
        P(DP),
    )
    return jax.shard_map(
        per_device,
        mesh=torus,
        in_specs=placed,
        out_specs=(P(DP, None), P(DP), P(DP)),
        check_vma=False,
    )
```
